32 devices in a mesh: gx: 2 (over y), gy: 4 (over x, core), gz: 4 (over z).
Axes of the slice: x: 2, y: 2, z: 4, core: 2. Of those that a mesh axis runs over, the one named last changes fastest.
Arguments:
- log_range: float32 [64, 128, 512], P('gx', 'gy', 'gz'), may hold values from 0.7 to 2
- state: float32 [2, 64, 128, 512], P(None, 'gx', 'gy', 'gz'), may hold values from -60 to 60, as said below
- adjoint_start: float32 [2, 64, 128, 512], P(None, 'gx', 'gy', 'gz'), may hold values from -0.3 to 0.3
- obs_index: int32 [2, 2, 4, 4, 4096], P(None, 'gx', 'gy', 'gz'), may hold values from 0 to 131071
- obs_value: float32 [2, 2, 4, 4, 4096], P(None, 'gx', 'gy', 'gz'), may hold values from -6 to 6
Outputs:
- gradient: float32 [64, 128, 512], P('gx', 'gy', 'gz')
- adjoint: float32 [2, 64, 128, 512], P(None, 'gx', 'gy', 'gz')
The draws below stay inside these ranges and needn't reach their ends.
Inputs may be any that keep to these rules, and one draw needn't show every extreme that they name: `obs_index`: each entry numbers a cell of its own device's block as (a * 32 + b) * 128 + c; cells may repeat. `state`: real values.
All inputs are finite; a program needn't handle non-finite values.
Results may differ from the reference program's by a relative error of at most 0.0001.
Values sent between devices are 32-bit elements; how exact they have to be, the bound alone decides.
A program may use at most 320 MiB of HBM per device.

```python
import jax
import jax.numpy as jnp

CX = 32
CY = 32
CZ = 128
NOBS = 4096
REPS = 2
ITERS = 4
NX = 64
NY = 128
NZ = 512
N_GX = 2
N_GY = 4
N_GZ = 4


def draw_state(key, part):
    along_x = (jnp.arange(NX, dtype=jnp.float32) / NX).reshape(-1, 1, 1)
    along_y = (jnp.arange(NY, dtype=jnp.float32) / NY).reshape(1, -1, 1)
    along_z = (jnp.arange(NZ, dtype=jnp.float32) / NZ).reshape(1, 1, -1)
    base = jnp.clip(jax.random.normal(key, (REPS, NX, NY, NZ), jnp.float32), -6.0, 6.0)
    spread = 3.0 ** along_x * 1.7 ** along_y * 1.7 ** along_z
    return base * spread[None]


def place_ends(drawn, rng, smallest, top_value):
    longest = drawn.shape.index(max(drawn.shape))
    spots = []
    for shift in (0, 1):
        where = [jax.random.randint(jax.random.fold_in(rng, axis), (), 0, length) for axis, length in enumerate(drawn.shape)]
        where[longest] = (where[longest] + shift) % drawn.shape[longest]
        spots.append(tuple(where))
    return drawn.at[spots[0]].set(smallest).at[spots[1]].set(top_value)


def block_levels(stream_key, dims, split, low, largest):
    level = 1.0
    for dim, blocks in split:
        draws = jax.random.uniform(jax.random.fold_in(jax.random.fold_in(stream_key, 6), dim), (blocks,), jnp.float32, low / len(split), largest / len(split))
        level = level * jnp.repeat(jnp.exp(draws), dims[dim] // blocks).reshape((-1,) + (1,) * (len(dims) - 1 - dim))
    return level


def scatter_about(rng, extent, deviation, limit, shards=(), kind=jnp.bfloat16):
    entries = deviation * jax.random.normal(rng, extent, jnp.float32)
    if shards:
        entries = entries * block_levels(rng, extent, shards, -0.22, 0.18)
    return jnp.clip(entries, -limit, limit).astype(kind)


def setup_inputs(seed: int = 0) -> dict:
    keys = jax.random.split(jax.random.key(seed), 6)
    log_range = jnp.clip(0.7 + 1.3 * jax.random.uniform(keys[0], (NX, NY, NZ), jnp.float32) ** block_levels(keys[0], (NX, NY, NZ), ((0, 2), (1, 4), (2, 4)), -0.2, 0.2), 0.7, 2.0)
    state = draw_state(jax.random.fold_in(keys[5], 71), 0)
    adjoint_start = scatter_about(keys[2], (REPS, NX, NY, NZ), 0.05, 0.3, ((1, 2), (2, 4), (3, 4)), jnp.float32)
    obs_index = place_ends(jax.random.randint(keys[3], (REPS, N_GX, N_GY, N_GZ, NOBS), 0, CX * CY * CZ), jax.random.fold_in(keys[3], 1), 0, (CX * CY * CZ) - 1).astype(jnp.int32)
    obs_value = scatter_about(keys[4], (REPS, N_GX, N_GY, N_GZ, NOBS), 1.0, 6.0, ((1, 2), (2, 4), (3, 4)), jnp.float32)
    return {"log_range": log_range, "state": state, "adjoint_start": adjoint_start, "obs_index": obs_index, "obs_value": obs_value}


noise_var = 0.25


def stencil(field, kappa_sq):
    beside = jnp.roll(field, -1, 0) + jnp.roll(field, 1, 0)
    beside = beside + jnp.roll(field, -1, 1) + jnp.roll(field, 1, 1)
    beside = beside + jnp.roll(field, -1, 2) + jnp.roll(field, 1, 2)
    return (kappa_sq + 6.0) * field - beside


def reference(log_range, state, adjoint_start, obs_index, obs_value):
    kappa_sq = 4.0 * jnp.exp(-2.0 * log_range)
    block_x = (jnp.arange(N_GX, dtype=jnp.int32) * CX).reshape(-1, 1, 1, 1)
    block_y = (jnp.arange(N_GY, dtype=jnp.int32) * CY).reshape(1, -1, 1, 1)
    block_z = (jnp.arange(N_GZ, dtype=jnp.int32) * CZ).reshape(1, 1, -1, 1)
    total = NX * NY * NZ
    gradient = jnp.zeros((NX, NY, NZ), jnp.float32)
    adjoints = []
    for replica in range(REPS):
        local = obs_index[replica].astype(jnp.int32)
        first = local // (CY * CZ) + block_x
        second = (local // CZ) % CY + block_y
        third = local % CZ + block_z
        global_cell = ((first * NY + second) * NZ + third).reshape(-1).astype(jnp.int32)
        field = state[replica]
        misfit = field.reshape(-1)[global_cell] - obs_value[replica].reshape(-1)
        obs_weight = jnp.zeros((total,), jnp.float32).at[global_cell].add(1.0 / noise_var).reshape(NX, NY, NZ)
        right_side = jnp.zeros((total,), jnp.float32).at[global_cell].add(-misfit / noise_var).reshape(NX, NY, NZ)

        def system(vector):
            return stencil(stencil(vector, kappa_sq), kappa_sq) + obs_weight * vector

        adjoint = adjoint_start[replica]
        residual = right_side - system(adjoint)
        direction = residual
        norm_now = jnp.sum(residual * residual)
        for iteration in range(ITERS):
            image = system(direction)
            step_size = norm_now / jnp.sum(direction * image)
            adjoint = adjoint + step_size * direction
            if iteration + 1 < ITERS:
                residual = residual - step_size * image
                norm_next = jnp.sum(residual * residual)
                direction = residual + (norm_next / norm_now) * direction
                norm_now = norm_next
        state_image = stencil(field, kappa_sq)
        adjoint_image = stencil(adjoint, kappa_sq)
        gradient = gradient + (-2.0 * kappa_sq * (adjoint * state_image + adjoint_image * field))
        adjoints.append(adjoint)
    return gradient, jnp.stack(adjoints, 0)
```

```python
import functools
import itertools

import jax
import jax.numpy as jnp
from jax import lax
from jax.experimental import pallas as pl
from jax.experimental.pallas import tpu as pltpu
from jax.sharding import PartitionSpec as P

ITERS = 4
LANES = 128
AXES = ("gx", "gy", "gz")
MESH = pl.DeviceIdType.MESH

noise_var = 0.25


def kernel(
    sizes, dims, lr_ref, state_ref, start_ref, idx_ref, val_ref, grad_ref, adj_ref,
    ext, ysend, yrecv, zsend, zrecv, kap, weight, values, rhs_hot, res, image,
    xi, ast, res_image, d, di, s_buf, z_buf, q_buf, red_out, red, send_sem, recv_sem, red_send, red_recv,
):
    sets, cx, cy, cz, nobs = dims
    rows = cx * cy
    place = [lax.axis_index(axis) for axis in AXES]
    rank = (place[0] * sizes[1] + place[1]) * sizes[2] + place[2]
    total = sizes[0] * sizes[1] * sizes[2]
    lane = lax.broadcasted_iota(jnp.int32, (cy, LANES), 1)
    row = lax.broadcasted_iota(jnp.int32, (cy, LANES), 0)
    small_lane = lax.broadcasted_iota(jnp.int32, (1, LANES), 1)
    offsets = [o for o in itertools.product(*[range(n) for n in sizes]) if any(o)]

    def device_at(offset):
        return tuple(lax.rem(p + o, n) for p, o, n in zip(place, offset, sizes))

    barrier = pltpu.get_barrier_semaphore()
    for offset in offsets:
        pl.semaphore_signal(barrier, inc=1, device_id=device_at(offset), device_id_type=MESH)

    def inner(x):
        return pl.ds(pl.multiple_of((x + 1) * cy, cy), cy)

    def plain(x):
        return pl.ds(pl.multiple_of(x * cy, cy), cy)

    def fold(v):
        return jnp.sum(v.reshape(cy // 8, 8, LANES), axis=0)

    def sweep(body, slot=None, sums=0):
        zero = jnp.zeros((cy, LANES), jnp.float32)
        faces = (zero, zero) if slot is not None else ()
        gathered = []
        for s in range(sets):
            def step(x, carry, s=s):
                faces, acc = carry
                slab, terms = body(s, x)
                if slot is not None:
                    at = s * cx + x
                    here = lane == at
                    low = jnp.where(here, pltpu.roll(slab, at, 1), faces[0])
                    high = jnp.where(here, pltpu.roll(slab, at + 1, 1), faces[1])
                    faces = (low, high)
                acc = tuple(a + fold(t) for a, t in zip(acc, terms))
                return faces, acc
            acc = tuple(jnp.zeros((8, LANES), jnp.float32) for _ in range(sums))
            faces, acc = lax.fori_loop(0, cx, step, (faces, acc), unroll=4)
            gathered.append(acc)
        if slot is not None:
            zsend[slot, 0] = faces[0]
            zsend[slot, 1] = faces[1]
            for s in range(sets):
                ysend[slot, 0, s * cx:(s + 1) * cx] = ext[slot, s, pl.ds(cy, cx, stride=cy), :]
                ysend[slot, 1, s * cx:(s + 1) * cx] = ext[slot, s, pl.ds(2 * cy - 1, cx, stride=cy), :]
        return gathered

    def copies(slot):
        near = [[tuple(sign if i == axis else 0 for i in range(3)) for sign in (-1, 1)] for axis in range(3)]
        ends = [
            (ext.at[slot, :, pl.ds(cy, cy), :], ext.at[slot, :, pl.ds((cx + 1) * cy, cy), :]),
            (ext.at[slot, :, pl.ds(cx * cy, cy), :], ext.at[slot, :, pl.ds(0, cy), :]),
            (ysend.at[slot, 0], yrecv.at[slot, 1]),
            (ysend.at[slot, 1], yrecv.at[slot, 0]),
            (zsend.at[slot, 0], zrecv.at[slot, 1]),
            (zsend.at[slot, 1], zrecv.at[slot, 0]),
        ]
        out = []
        for n, (src, dst) in enumerate(ends):
            offset = tuple(o % size for o, size in zip(near[n // 2][n % 2], sizes))
            out.append(pltpu.make_async_remote_copy(
                src_ref=src, dst_ref=dst, send_sem=send_sem.at[slot, n], recv_sem=recv_sem.at[slot, n],
                device_id=device_at(offset), device_id_type=MESH))
        return out

    def send(slot):
        for copy in copies(slot):
            copy.start()

    def arrive(slot):
        for copy in copies(slot):
            copy.wait()

    def apply(slot, s, x):
        center = ext[slot, s, inner(x), :]
        beside = ext[slot, s, inner(x + 1), :] + ext[slot, s, inner(x - 1), :]
        before = yrecv[slot, 0, pl.ds(s * cx + x, 1), :]
        after = yrecv[slot, 1, pl.ds(s * cx + x, 1), :]
        beside = beside + jnp.where(row == cy - 1, after, pltpu.roll(center, cy - 1, 0))
        beside = beside + jnp.where(row == 0, before, pltpu.roll(center, 1, 0))
        turn = LANES - 1 - (s * cx + x)
        low = pltpu.roll(zrecv[slot, 0], turn, 1)
        high = pltpu.roll(zrecv[slot, 1], turn + 1, 1)
        beside = beside + pltpu.roll(jnp.where(lane == 0, high, center), LANES - 1, 1)
        beside = beside + pltpu.roll(jnp.where(lane == LANES - 1, low, center), 1, 1)
        return (kap[plain(x), :] + 6.0) * center - beside

    def reduce_start(n, gathered):
        line = jnp.zeros((1, LANES), jnp.float32)
        for s in range(sets):
            for j in range(2):
                value = jnp.sum(jnp.sum(gathered[s][j], axis=0, keepdims=True), axis=1, keepdims=True)
                line = jnp.where(small_lane == 2 * s + j, value, line)
        red_out[n] = line
        red[n, rank] = line
        for offset in offsets:
            pltpu.make_async_remote_copy(
                src_ref=red_out.at[n], dst_ref=red.at[n, rank], send_sem=red_send.at[n],
                recv_sem=red_recv.at[n], device_id=device_at(offset), device_id_type=MESH).start()

    def reduce_end(n):
        many = red.at[n, pl.ds(0, total - 1)]
        pltpu.make_async_copy(many, many, red_recv.at[n]).wait()
        pltpu.make_async_copy(many, many, red_send.at[n]).wait()
        line = jnp.sum(red[n], axis=0)
        def pick(j):
            value = jnp.sum(jnp.where(small_lane == j, line, 0.0), axis=1, keepdims=True)
            return jnp.broadcast_to(value, (1, LANES))
        return [(pick(2 * s), pick(2 * s + 1)) for s in range(sets)]

    def load(slot, ref):
        def body(s, x):
            slab = ref[s, plain(x), :]
            ext[slot, s, inner(x), :] = slab
            return slab, ()
        sweep(body, slot)

    load(0, start_ref)
    load(2, state_ref)
    pl.semaphore_wait(barrier, total - 1)
    send(0)
    send(2)

    kap[...] = 4.0 * jnp.exp(-2.0 * lr_ref[...])

    tile = min(rows, 256)
    hot_lane = lax.broadcasted_iota(jnp.int32, (LANES, nobs), 0)
    for s in range(sets):
        cell = idx_ref[s:s + 1, :]
        value = val_ref[s:s + 1, :]
        hit = hot_lane == cell % cz
        top = value.astype(jnp.bfloat16).astype(jnp.float32)
        rhs_hot[0:LANES] = jnp.where(hit, 1.0, 0.0).astype(jnp.bfloat16)
        rhs_hot[LANES:2 * LANES] = jnp.where(hit, top, 0.0).astype(jnp.bfloat16)
        rhs_hot[2 * LANES:] = jnp.where(hit, value - top, 0.0).astype(jnp.bfloat16)
        line = cell // cz

        def step(m, carry, s=s, line=line):
            base = m * tile
            ids = lax.broadcasted_iota(jnp.int32, (tile, nobs), 0) + base
            hot = jnp.where(ids == line, 1.0, 0.0).astype(jnp.bfloat16)
            got = lax.dot_general(hot, rhs_hot[...], (((1,), (1,)), ((), ())), preferred_element_type=jnp.float32)
            at = pl.ds(pl.multiple_of(base, tile), tile)
            weight[s, at, :] = got[:, :LANES] * (1.0 / noise_var)
            values[s, at, :] = (got[:, LANES:2 * LANES] + got[:, 2 * LANES:]) * (1.0 / noise_var)
            return carry
        lax.fori_loop(0, rows // tile, step, 0)

    def start_pass(s, x):
        out = apply(0, s, x)
        ext[1, s, inner(x), :] = out
        xi[s, plain(x), :] = out
        return out, ()

    arrive(0)
    sweep(start_pass, 1)
    send(1)

    def right_pass(s, x):
        at = plain(x)
        right = values[s, at, :] - weight[s, at, :] * (state_ref[s, at, :] + start_ref[s, at, :])
        res[s, at, :] = right
        return right, ()

    sweep(right_pass)
    arrive(1)

    def residual_pass(s, x):
        out = res[s, plain(x), :] - apply(1, s, x)
        res[s, plain(x), :] = out
        ext[0, s, inner(x), :] = out
        return out, ()

    sweep(residual_pass, 0)
    send(0)

    def state_pass(s, x):
        out = apply(2, s, x)
        ast[s, plain(x), :] = out
        return out, ()

    arrive(2)
    sweep(state_pass)
    arrive(0)

    def inner_pass(s, x):
        out = apply(0, s, x)
        ext[1, s, inner(x), :] = out
        res_image[s, plain(x), :] = out
        return out, ()

    sweep(inner_pass, 1)
    send(1)
    arrive(1)

    def image_pass(s, x):
        now = res[s, plain(x), :]
        out = apply(1, s, x) + weight[s, plain(x), :] * now
        ext[0, s, inner(x), :] = out
        return out, (now * now, now * out)

    gathered = sweep(image_pass, 0, 2)
    send(0)
    reduce_start(0, gathered)

    def next_inner(s, x):
        out = apply(0, s, x)
        ext[1, s, inner(x), :] = out
        return out, ()

    def next_image(s, x):
        out = apply(1, s, x) + weight[s, plain(x), :] * ext[0, s, inner(x), :]
        image[s, plain(x), :] = out
        return out, ()

    norms = steps = None
    for k in range(ITERS):
        last = k + 1 == ITERS
        if not last:
            arrive(0)
            sweep(next_inner, 1)
            send(1)
            arrive(1)
            sweep(next_image)
        sums = reduce_end(k)
        if k == 0:
            ratio = None
            step_size = [norm / product for norm, product in sums]
        else:
            ratio = [sums[s][0] / norms[s] for s in range(sets)]
            step_size = [sums[s][0] / (sums[s][1] - ratio[s] * sums[s][0] / steps[s]) for s in range(sets)]
        norms, steps = [norm for norm, product in sums], step_size

        def follow(buf, s, at, new, ratio=ratio):
            if ratio is not None:
                new = new + ratio[s] * buf[s, at, :]
            return new

        if last:
            def finish(x, carry):
                at = plain(x)
                grad = jnp.zeros((cy, LANES), jnp.float32)
                for s in range(sets):
                    adj = adj_ref[s, at, :] + step_size[s] * follow(d, s, at, res[s, at, :])
                    adj_ref[s, at, :] = adj
                    applied = xi[s, at, :] + step_size[s] * follow(di, s, at, res_image[s, at, :])
                    grad = grad + (adj * ast[s, at, :] + applied * state_ref[s, at, :])
                grad_ref[at, :] = -2.0 * kap[at, :] * grad
                return carry
            lax.fori_loop(0, cx, finish, 0, unroll=2)
            break

        def update(s, x):
            at = plain(x)
            now, vec = res[s, at, :], ext[0, s, inner(x), :]
            z_new = follow(z_buf, s, at, image[s, at, :])
            s_new = follow(s_buf, s, at, vec)
            d[s, at, :] = follow(d, s, at, now)
            z_buf[s, at, :] = z_new
            s_buf[s, at, :] = s_new
            vec = vec - step_size[s] * z_new
            now = now - step_size[s] * s_new
            ext[0, s, inner(x), :] = vec
            res[s, at, :] = now
            return vec, (now * now, now * vec)

        more = k + 2 < ITERS
        gathered = sweep(update, 0 if more else None, 2)
        if more:
            send(0)
        reduce_start(k + 1, gathered)

        def trail(s, x):
            at = plain(x)
            base = start_ref if k == 0 else adj_ref
            adj_ref[s, at, :] = base[s, at, :] + step_size[s] * d[s, at, :]
            di_new = follow(di, s, at, res_image[s, at, :])
            di[s, at, :] = di_new
            xi[s, at, :] = xi[s, at, :] + step_size[s] * di_new
            q_new = follow(q_buf, s, at, ext[1, s, inner(x), :])
            q_buf[s, at, :] = q_new
            res_image[s, at, :] = res_image[s, at, :] - step_size[s] * q_new
            return q_new, ()

        sweep(trail)


def on_device(sizes, log_range, state, adjoint_start, obs_index, obs_value):
    sets, cx, cy, cz = state.shape
    nobs = obs_index.shape[-1]
    rows = cx * cy
    total = sizes[0] * sizes[1] * sizes[2]
    field = pltpu.VMEM((sets, rows, cz), jnp.float32)
    vmem = pl.BlockSpec(memory_space=pltpu.VMEM)
    gradient, adjoint = pl.pallas_call(
        functools.partial(kernel, sizes, (sets, cx, cy, cz, nobs)),
        out_shape=(
            jax.ShapeDtypeStruct((rows, cz), jnp.float32),
            jax.ShapeDtypeStruct((sets, rows, cz), jnp.float32),
        ),
        in_specs=[vmem] * 5,
        out_specs=(vmem, vmem),
        scratch_shapes=[
            pltpu.VMEM((3, sets, rows + 2 * cy, cz), jnp.float32),
            pltpu.VMEM((3, 2, sets * cx, cz), jnp.float32),
            pltpu.VMEM((3, 2, sets * cx, cz), jnp.float32),
            pltpu.VMEM((3, 2, cy, LANES), jnp.float32),
            pltpu.VMEM((3, 2, cy, LANES), jnp.float32),
            pltpu.VMEM((rows, cz), jnp.float32),
            field,
            field,
            pltpu.VMEM((3 * LANES, nobs), jnp.bfloat16),
            *([field] * 10),
            pltpu.VMEM((ITERS, 1, LANES), jnp.float32),
            pltpu.VMEM((ITERS, total, 1, LANES), jnp.float32),
            pltpu.SemaphoreType.DMA((3, 6)),
            pltpu.SemaphoreType.DMA((3, 6)),
            pltpu.SemaphoreType.DMA((ITERS,)),
            pltpu.SemaphoreType.DMA((ITERS,)),
        ],
        compiler_params=pltpu.CompilerParams(
            collective_id=0, has_side_effects=True, vmem_limit_bytes=60 * 1024 * 1024
        ),
    )(
        log_range.reshape(rows, cz),
        state.reshape(sets, rows, cz),
        adjoint_start.reshape(sets, rows, cz),
        obs_index.reshape(sets, nobs),
        obs_value.reshape(sets, nobs),
    )
    return gradient.reshape(cx, cy, cz), adjoint.reshape(sets, cx, cy, cz)


def solution(mesh):
    in_specs = (
        P("gx", "gy", "gz"),
        P(None, "gx", "gy", "gz"),
        P(None, "gx", "gy", "gz"),
        P(None, "gx", "gy", "gz", None),
        P(None, "gx", "gy", "gz", None),
    )
    out_specs = (P("gx", "gy", "gz"), P(None, "gx", "gy", "gz"))
    sizes = tuple(mesh.shape[axis] for axis in AXES)
    return jax.shard_map(
        functools.partial(on_device, sizes), mesh=mesh, in_specs=in_specs, out_specs=out_specs, check_vma=False
    )
```

```python
import functools
import itertools

import jax
import jax.numpy as jnp
from jax import lax
from jax.experimental import pallas as pl
from jax.experimental.pallas import tpu as pltpu
from jax.sharding import PartitionSpec as P

ITERS = 4
LANES = 128
AXES = ("gx", "gy", "gz")
MESH = pl.DeviceIdType.MESH

noise_var = 0.25


def kernel(
    sizes, dims, lr_ref, state_ref, start_ref, idx_ref, val_ref, grad_ref, adj_ref,
    ext, ysend, yrecv, zsend, zrecv, zboth, kap, weight, values, rhs_hot, res, image,
    xi, ast, res_image, d, di, s_buf, z_buf, q_buf, red_out, red, send_sem, recv_sem, red_send, red_recv,
):
    sets, cx, cy, cz, nobs = dims
    rows = cx * cy
    place = [lax.axis_index(axis) for axis in AXES]
    rank = (place[0] * sizes[1] + place[1]) * sizes[2] + place[2]
    total = sizes[0] * sizes[1] * sizes[2]
    lane = lax.broadcasted_iota(jnp.int32, (cy, LANES), 1)
    row = lax.broadcasted_iota(jnp.int32, (cy, LANES), 0)
    pair = lane // 2
    even = lane % 2 == 0
    small_lane = lax.broadcasted_iota(jnp.int32, (1, LANES), 1)
    offsets = [o for o in itertools.product(*[range(n) for n in sizes]) if any(o)]

    def device_at(offset):
        return tuple(lax.rem(p + o, n) for p, o, n in zip(place, offset, sizes))

    barrier = pltpu.get_barrier_semaphore()
    for offset in offsets:
        pl.semaphore_signal(barrier, inc=1, device_id=device_at(offset), device_id_type=MESH)

    def inner(x):
        return pl.ds(pl.multiple_of((x + 1) * cy, cy), cy)

    def plain(x):
        return pl.ds(pl.multiple_of(x * cy, cy), cy)

    def fold(v):
        return jnp.sum(v.reshape(cy // 8, 8, LANES), axis=0)

    def sweep(body, slot=None, sums=0):
        zero = jnp.zeros((cy, LANES), jnp.float32)
        faces = (zero,) * sets if slot is not None else ()

        def step(x, carry):
            faces, gathered = carry
            packed, added = [], []
            for s in range(sets):
                slab, terms = body(s, x)
                if slot is not None:
                    at = s * cx + x
                    packed.append(jnp.where(pair == at, pltpu.roll(slab, 2 * at + 1, 1), faces[s]))
                added.append(tuple(a + fold(t) for a, t in zip(gathered[s], terms)))
            return tuple(packed), tuple(added)

        start = tuple(tuple(jnp.zeros((8, LANES), jnp.float32) for _ in range(sums)) for _ in range(sets))
        faces, gathered = lax.fori_loop(0, cx, step, (faces, start), unroll=8)
        if slot is not None:
            zsend[slot] = functools.reduce(jnp.add, faces)
            for s in range(sets):
                ysend[slot, 0, s * cx:(s + 1) * cx] = ext[slot, s, pl.ds(cy, cx, stride=cy), :]
                ysend[slot, 1, s * cx:(s + 1) * cx] = ext[slot, s, pl.ds(2 * cy - 1, cx, stride=cy), :]
        return gathered

    def copies(slot):
        near = [[tuple(sign if i == axis else 0 for i in range(3)) for sign in (-1, 1)] for axis in range(3)]
        ends = [
            (ext.at[slot, :, pl.ds(cy, cy), :], ext.at[slot, :, pl.ds((cx + 1) * cy, cy), :]),
            (ext.at[slot, :, pl.ds(cx * cy, cy), :], ext.at[slot, :, pl.ds(0, cy), :]),
            (ysend.at[slot, 0], yrecv.at[slot, 1]),
            (ysend.at[slot, 1], yrecv.at[slot, 0]),
            (zsend.at[slot], zrecv.at[slot, 1]),
            (zsend.at[slot], zrecv.at[slot, 0]),
        ]
        out = []
        for n, (src, dst) in enumerate(ends):
            offset = tuple(o % size for o, size in zip(near[n // 2][n % 2], sizes))
            out.append(pltpu.make_async_remote_copy(
                src_ref=src, dst_ref=dst, send_sem=send_sem.at[slot, n], recv_sem=recv_sem.at[slot, n],
                device_id=device_at(offset), device_id_type=MESH))
        return out

    def send(slot):
        for copy in copies(slot):
            copy.start()

    def arrive(slot):
        for copy in copies(slot):
            copy.wait()
        zboth[slot] = jnp.where(even, zrecv[slot, 0], pltpu.roll(zrecv[slot, 1], LANES - 2, 1))

    def apply(slot, s, x):
        center = ext[slot, s, inner(x), :]
        beside = ext[slot, s, inner(x + 1), :] + ext[slot, s, inner(x - 1), :]
        before = yrecv[slot, 0, pl.ds(s * cx + x, 1), :]
        after = yrecv[slot, 1, pl.ds(s * cx + x, 1), :]
        base = (x + 1) * cy
        beside = beside + jnp.where(row == cy - 1, after, pltpu.roll(center, cy - 1, 0))
        beside = beside + jnp.where(row == 0, before, pltpu.roll(center, 1, 0))
        edge = pltpu.roll(zboth[slot], lax.rem(LANES - 2 * (s * cx + x), LANES), 1)
        beside = beside + jnp.where(lane == LANES - 1, edge, pltpu.roll(center, LANES - 1, 1))
        beside = beside + jnp.where(lane == 0, edge, pltpu.roll(center, 1, 1))
        return (kap[plain(x), :] + 6.0) * center - beside

    def reduce_start(n, gathered):
        line = jnp.zeros((1, LANES), jnp.float32)
        for s in range(sets):
            for j in range(2):
                value = jnp.sum(jnp.sum(gathered[s][j], axis=0, keepdims=True), axis=1, keepdims=True)
                line = jnp.where(small_lane == 2 * s + j, value, line)
        red_out[n] = line
        red[n, rank] = line
        for offset in offsets:
            pltpu.make_async_remote_copy(
                src_ref=red_out.at[n], dst_ref=red.at[n, rank], send_sem=red_send.at[n],
                recv_sem=red_recv.at[n], device_id=device_at(offset), device_id_type=MESH).start()

    def reduce_end(n):
        many = red.at[n, pl.ds(0, total - 1)]
        pltpu.make_async_copy(many, many, red_recv.at[n]).wait()
        pltpu.make_async_copy(many, many, red_send.at[n]).wait()
        line = jnp.sum(red[n], axis=0)
        def pick(j):
            value = jnp.sum(jnp.where(small_lane == j, line, 0.0), axis=1, keepdims=True)
            return jnp.broadcast_to(value, (1, LANES))
        return [(pick(2 * s), pick(2 * s + 1)) for s in range(sets)]

    def load(slot, ref):
        def body(s, x):
            slab = ref[s, plain(x), :]
            ext[slot, s, inner(x), :] = slab
            return slab, ()
        sweep(body, slot)

    load(0, start_ref)
    load(2, state_ref)
    pl.semaphore_wait(barrier, total - 1)
    send(0)
    send(2)

    kap[...] = 4.0 * jnp.exp(-2.0 * lr_ref[...])

    tile = min(rows, 256)
    hot_lane = lax.broadcasted_iota(jnp.int32, (LANES, nobs), 0)
    for s in range(sets):
        cell = idx_ref[s:s + 1, :]
        value = val_ref[s:s + 1, :]
        hit = hot_lane == cell % cz
        top = value.astype(jnp.bfloat16).astype(jnp.float32)
        rhs_hot[0:LANES] = jnp.where(hit, 1.0, 0.0).astype(jnp.bfloat16)
        rhs_hot[LANES:2 * LANES] = jnp.where(hit, top, 0.0).astype(jnp.bfloat16)
        rhs_hot[2 * LANES:] = jnp.where(hit, value - top, 0.0).astype(jnp.bfloat16)
        line = cell // cz

        def step(m, carry, s=s, line=line):
            base = m * tile
            ids = lax.broadcasted_iota(jnp.int32, (tile, nobs), 0) + base
            hot = jnp.where(ids == line, 1.0, 0.0).astype(jnp.bfloat16)
            got = lax.dot_general(hot, rhs_hot[...], (((1,), (1,)), ((), ())), preferred_element_type=jnp.float32)
            at = pl.ds(pl.multiple_of(base, tile), tile)
            weight[s, at, :] = got[:, :LANES] * (1.0 / noise_var)
            values[s, at, :] = (got[:, LANES:2 * LANES] + got[:, 2 * LANES:]) * (1.0 / noise_var)
            return carry
        lax.fori_loop(0, rows // tile, step, 0)

    def start_pass(s, x):
        out = apply(0, s, x)
        ext[1, s, inner(x), :] = out
        xi[s, plain(x), :] = out
        return out, ()

    arrive(0)
    sweep(start_pass, 1)
    send(1)

    def right_pass(s, x):
        at = plain(x)
        right = values[s, at, :] - weight[s, at, :] * (state_ref[s, at, :] + start_ref[s, at, :])
        res[s, at, :] = right
        return right, ()

    sweep(right_pass)
    arrive(1)

    def residual_pass(s, x):
        out = res[s, plain(x), :] - apply(1, s, x)
        res[s, plain(x), :] = out
        ext[0, s, inner(x), :] = out
        return out, ()

    sweep(residual_pass, 0)
    send(0)

    def state_pass(s, x):
        out = apply(2, s, x)
        ast[s, plain(x), :] = out
        return out, ()

    arrive(2)
    sweep(state_pass)
    arrive(0)

    def inner_pass(s, x):
        out = apply(0, s, x)
        ext[1, s, inner(x), :] = out
        res_image[s, plain(x), :] = out
        return out, ()

    sweep(inner_pass, 1)
    send(1)
    arrive(1)

    def image_pass(s, x):
        now = res[s, plain(x), :]
        out = apply(1, s, x) + weight[s, plain(x), :] * now
        ext[0, s, inner(x), :] = out
        return out, (now * now, now * out)

    gathered = sweep(image_pass, 0, 2)
    send(0)
    reduce_start(0, gathered)

    def next_inner(s, x):
        out = apply(0, s, x)
        ext[1, s, inner(x), :] = out
        return out, ()

    def next_image(s, x):
        out = apply(1, s, x) + weight[s, plain(x), :] * ext[0, s, inner(x), :]
        image[s, plain(x), :] = out
        return out, ()

    norms = steps = None
    for k in range(ITERS):
        last = k + 1 == ITERS
        if not last:
            arrive(0)
            sweep(next_inner, 1)
            send(1)
            arrive(1)
            sweep(next_image)
        sums = reduce_end(k)
        if k == 0:
            ratio = None
            step_size = [norm / product for norm, product in sums]
        else:
            ratio = [sums[s][0] / norms[s] for s in range(sets)]
            step_size = [sums[s][0] / (sums[s][1] - ratio[s] * sums[s][0] / steps[s]) for s in range(sets)]
        norms, steps = [norm for norm, product in sums], step_size

        def follow(buf, s, at, new, ratio=ratio):
            if ratio is not None:
                new = new + ratio[s] * buf[s, at, :]
            return new

        if last:
            def finish(x, carry):
                at = plain(x)
                grad = jnp.zeros((cy, LANES), jnp.float32)
                for s in range(sets):
                    adj = adj_ref[s, at, :] + step_size[s] * follow(d, s, at, res[s, at, :])
                    adj_ref[s, at, :] = adj
                    applied = xi[s, at, :] + step_size[s] * follow(di, s, at, res_image[s, at, :])
                    grad = grad + (adj * ast[s, at, :] + applied * state_ref[s, at, :])
                grad_ref[at, :] = -2.0 * kap[at, :] * grad
                return carry
            lax.fori_loop(0, cx, finish, 0, unroll=8)
            break

        def update(s, x):
            at = plain(x)
            now, vec = res[s, at, :], ext[0, s, inner(x), :]
            z_new = follow(z_buf, s, at, image[s, at, :])
            s_new = follow(s_buf, s, at, vec)
            d[s, at, :] = follow(d, s, at, now)
            z_buf[s, at, :] = z_new
            s_buf[s, at, :] = s_new
            vec = vec - step_size[s] * z_new
            now = now - step_size[s] * s_new
            ext[0, s, inner(x), :] = vec
            res[s, at, :] = now
            return vec, (now * now, now * vec)

        more = k + 2 < ITERS
        gathered = sweep(update, 0 if more else None, 2)
        if more:
            send(0)
        reduce_start(k + 1, gathered)

        def trail(s, x):
            at = plain(x)
            base = start_ref if k == 0 else adj_ref
            adj_ref[s, at, :] = base[s, at, :] + step_size[s] * d[s, at, :]
            di_new = follow(di, s, at, res_image[s, at, :])
            di[s, at, :] = di_new
            xi[s, at, :] = xi[s, at, :] + step_size[s] * di_new
            q_new = follow(q_buf, s, at, ext[1, s, inner(x), :])
            q_buf[s, at, :] = q_new
            res_image[s, at, :] = res_image[s, at, :] - step_size[s] * q_new
            return q_new, ()

        sweep(trail)


def on_device(sizes, log_range, state, adjoint_start, obs_index, obs_value):
    sets, cx, cy, cz = state.shape
    nobs = obs_index.shape[-1]
    rows = cx * cy
    total = sizes[0] * sizes[1] * sizes[2]
    field = pltpu.VMEM((sets, rows, cz), jnp.float32)
    vmem = pl.BlockSpec(memory_space=pltpu.VMEM)
    gradient, adjoint = pl.pallas_call(
        functools.partial(kernel, sizes, (sets, cx, cy, cz, nobs)),
        out_shape=(
            jax.ShapeDtypeStruct((rows, cz), jnp.float32),
            jax.ShapeDtypeStruct((sets, rows, cz), jnp.float32),
        ),
        in_specs=[vmem] * 5,
        out_specs=(vmem, vmem),
        scratch_shapes=[
            pltpu.VMEM((3, sets, rows + 2 * cy, cz), jnp.float32),
            pltpu.VMEM((3, 2, sets * cx, cz), jnp.float32),
            pltpu.VMEM((3, 2, sets * cx, cz), jnp.float32),
            pltpu.VMEM((3, cy, LANES), jnp.float32),
            pltpu.VMEM((3, 2, cy, LANES), jnp.float32),
            pltpu.VMEM((3, cy, LANES), jnp.float32),
            pltpu.VMEM((rows, cz), jnp.float32),
            field,
            field,
            pltpu.VMEM((3 * LANES, nobs), jnp.bfloat16),
            *([field] * 10),
            pltpu.VMEM((ITERS, 1, LANES), jnp.float32),
            pltpu.VMEM((ITERS, total, 1, LANES), jnp.float32),
            pltpu.SemaphoreType.DMA((3, 6)),
            pltpu.SemaphoreType.DMA((3, 6)),
            pltpu.SemaphoreType.DMA((ITERS,)),
            pltpu.SemaphoreType.DMA((ITERS,)),
        ],
        compiler_params=pltpu.CompilerParams(
            collective_id=0, has_side_effects=True, vmem_limit_bytes=60 * 1024 * 1024
        ),
    )(
        log_range.reshape(rows, cz),
        state.reshape(sets, rows, cz),
        adjoint_start.reshape(sets, rows, cz),
        obs_index.reshape(sets, nobs),
        obs_value.reshape(sets, nobs),
    )
    return gradient.reshape(cx, cy, cz), adjoint.reshape(sets, cx, cy, cz)


def solution(mesh):
    in_specs = (
        P("gx", "gy", "gz"),
        P(None, "gx", "gy", "gz"),
        P(None, "gx", "gy", "gz"),
        P(None, "gx", "gy", "gz", None),
        P(None, "gx", "gy", "gz", None),
    )
    out_specs = (P("gx", "gy", "gz"), P(None, "gx", "gy", "gz"))
    sizes = tuple(mesh.shape[axis] for axis in AXES)
    return jax.shard_map(
        functools.partial(on_device, sizes), mesh=mesh, in_specs=in_specs, out_specs=out_specs, check_vma=False
    )
```
